128 devices in a mesh: row: 8 (over z, x_hi), col: 16 (over y, x_lo, core).
Axes of the slice: x: 4 (x_hi: 2, x_lo: 2; x = x_hi * 2 + x_lo), y: 4, z: 4, core: 2. Of those that a mesh axis runs over, the one named last changes fastest.
Arguments:
- node_feats: bfloat16 [16384, 512], P(('row', 'col')), may hold values from -80 to 80
- block_mask: int32 [128, 128], replicated, may hold values from 0 to 1, as said below
- w_qkv: bfloat16 [2, 512, 1536], replicated, may hold values from -0.25 to 0.25
- w_out: bfloat16 [2, 512, 512], replicated, may hold values from -0.79296875 to 0.79296875
- w_up: bfloat16 [2, 512, 1024], replicated, may hold values from -0.25 to 0.25
- w_down: bfloat16 [2, 1024, 512], replicated, may hold values from -0.1875 to 0.1875
- ln_gain: float32 [2, 2, 512], replicated, may hold values from 0.1 to 1.9
- ln_bias: float32 [2, 2, 512], replicated, may hold values from -3 to 3
Outputs:
- nodes_out: bfloat16 [16384, 512], P(('row', 'col'))
The draws below stay inside these ranges and needn't reach their ends.
Inputs may be any that keep to these rules, and one draw needn't show every extreme that they name: `block_mask`: A symmetric 0/1 table over the 128 node blocks; every block is linked with itself.
All inputs are finite; a program needn't handle non-finite values.
Results may differ from the reference program's by a relative error of at most 0.022.
Values may be sent and summed in bfloat16 or wider, within the bound.
A program may use at most 128 MiB of HBM per device.

```python
import jax
import jax.numpy as jnp
from jax import lax

D = 512
HEADS = 8
FF = 1024
BLOCK = 128
LAYERS = 2
NB = 128
NODES = 16384
N_ROW = 8


def draw_node_feats(key, part):
    base = jnp.clip(jax.random.normal(key, (NODES, D), jnp.float32), -6.0, 6.0)
    return base.astype(jnp.bfloat16)


def draw_block_mask(key, part):
    index = jnp.arange(NB, dtype=jnp.int32)
    apart = jnp.abs(index[:, None] - index[None, :])
    apart = jnp.minimum(apart, NB - apart)
    random_bits = jax.random.randint(key, (NB, NB), 0, 16, dtype=jnp.int32)
    busy = jax.random.randint(jax.random.fold_in(key, 1), (NB,), 0, 8, dtype=jnp.int32) == 0
    far_row = NB // 2
    far_col = NB // (2 * N_ROW)
    limit = jnp.where(apart <= 1, 12, jnp.where(apart <= 3, 3, 0))
    limit = jnp.where(busy[:, None] | busy[None, :], jnp.maximum(limit, 2), limit)
    limit = jnp.where((apart == far_row) | (apart == far_col), 16, limit)
    upper = random_bits < limit
    linked = upper | upper.T | (apart == 0)
    return linked.astype(jnp.int32)


def scatter_about(rng, dims, scale, most, kind=jnp.bfloat16):
    array = scale * jax.random.normal(rng, dims, jnp.float32)
    return jnp.clip(array, min=-most, max=most).astype(kind)


def setup_inputs(seed: int = 0) -> dict:
    key_of = jax.random.split(jax.random.key(seed), 9)
    return {
        "node_feats": draw_node_feats(jax.random.fold_in(key_of[8], 71), 0),
        "block_mask": draw_block_mask(jax.random.fold_in(key_of[8], 71), 0),
        "w_qkv": scatter_about(key_of[2], (LAYERS, D, 3 * D), D ** -0.5, 0.25),
        "w_out": scatter_about(key_of[3], (LAYERS, D, D), (3.0 * D ** -0.5), 0.79296875),
        "w_up": scatter_about(key_of[4], (LAYERS, D, FF), D ** -0.5, 0.25),
        "w_down": scatter_about(key_of[5], (LAYERS, FF, D), FF ** -0.5, 0.1875),
        "ln_gain": jnp.clip(1.0 + 0.18 * jax.random.normal(key_of[6], (LAYERS, 2, D), jnp.float32), 0.1, 1.9),
        "ln_bias": scatter_about(key_of[7], (LAYERS, 2, D), 0.5, 3.0, jnp.float32),
    }


def layer_norm(values, gain, bias):
    center = values - lax.optimization_barrier(jnp.mean(values, axis=-1, keepdims=True))
    spread = lax.optimization_barrier(jnp.mean(center * center, axis=-1, keepdims=True))
    return center * lax.rsqrt(spread + 1e-05) * gain + bias

def attend(queries, keys, values, block_mask):
    head_dim = D // HEADS
    qrows = 512
    qsplit = queries.astype(jnp.float32).reshape(NODES // qrows, qrows, HEADS, head_dim)
    ksplit = keys.astype(jnp.float32).reshape(NODES, HEADS, head_dim)
    vsplit = values.astype(jnp.float32).reshape(NODES, HEADS, head_dim)
    mask_rows = block_mask.reshape(NODES // qrows, qrows // BLOCK, NB)

    def one_block(item):
        qblock, mblock = item
        scores = jnp.einsum('qhd,khd->hqk', qblock, ksplit) * (1.0 / head_dim ** 0.5)
        allowed = (jnp.repeat(jnp.repeat(mblock, BLOCK, axis=0), BLOCK, axis=1) > 0)[None]
        peak = lax.optimization_barrier(jnp.max(jnp.where(allowed, scores, -1e+30), axis=-1, keepdims=True))
        weights = jnp.where(allowed, jnp.exp(scores - peak), 0.0)
        mass = lax.optimization_barrier(jnp.sum(weights, axis=-1))
        rounded = lax.optimization_barrier(weights.astype(jnp.bfloat16)).astype(jnp.float32)
        summed = jnp.einsum('hqk,khd->qhd', rounded, vsplit)
        return (summed / mass.T[:, :, None]).reshape(qrows, D).astype(jnp.bfloat16)
    return lax.map(one_block, (qsplit, mask_rows)).reshape(NODES, D)

def reference(node_feats, block_mask, w_qkv, w_out, w_up, w_down, ln_gain, ln_bias):
    x = node_feats
    for layer in range(LAYERS):
        qkv = jnp.dot(x, w_qkv[layer], preferred_element_type=jnp.float32).astype(jnp.bfloat16)
        attn = attend(qkv[:, :D], qkv[:, D:2 * D], qkv[:, 2 * D:], block_mask)
        mixed = jnp.dot(attn, w_out[layer], preferred_element_type=jnp.float32)
        hidden = layer_norm(x.astype(jnp.float32) + mixed, ln_gain[layer, 0], ln_bias[layer, 0]).astype(jnp.bfloat16)
        up = jax.nn.gelu(jnp.dot(hidden, w_up[layer], preferred_element_type=jnp.float32)).astype(jnp.bfloat16)
        down = jnp.dot(up, w_down[layer], preferred_element_type=jnp.float32)
        x = layer_norm(hidden.astype(jnp.float32) + down, ln_gain[layer, 1], ln_bias[layer, 1]).astype(jnp.bfloat16)
    return x
```

```python
import functools
import math

import jax
import jax.numpy as jnp
from jax import lax
from jax.experimental import pallas as pl
from jax.experimental.pallas import tpu as pltpu
from jax.sharding import PartitionSpec as P

HEADS = 8
F32, BF16 = jnp.float32, jnp.bfloat16
FLOOR = -1e30
MESH = pl.DeviceIdType.MESH
OFFS = (0, -1, 1, 2)
ORDER = ((0, 0), (1, 0), (2, 0), (0, 1), (0, 2), (3, 0), (1, 1), (1, 2), (2, 1), (2, 2), (0, 3),
         (3, 1), (3, 2), (1, 3), (2, 3), (3, 3))
UNROLL = 4


def layer_norm(values, gain, bias):
    center = values - jnp.mean(values, axis=-1, keepdims=True)
    spread = jnp.mean(center * center, axis=-1, keepdims=True)
    return center * lax.rsqrt(spread + 1e-05) * gain + bias


def gelu(v):
    inner = math.sqrt(2.0 / math.pi) * (v + 0.044715 * (v * v * v))
    return v * (0.5 * (1.0 + jnp.tanh(inner)))


def coords():
    row, col = lax.axis_index("row"), lax.axis_index("col")
    return (row % 2) * 2 + (col // 2) % 2, col // 4, row // 2, col % 2


def dev(x, y, z, c):
    return {"row": z * 2 + x // 2, "col": y * 4 + (x % 2) * 2 + c}


def exchange(l, first, last, *refs):
    refs = list(refs)
    take = refs.pop
    x_in = take(0)
    if not first:
        pin, sin = take(0), take(0)
    hqkv = None if last else take(0)
    if not first:
        hout, hup, hdown, gain, bias = (take(0) for _ in range(5))
    if last:
        x_out = take(0)
    else:
        kbuf, vbuf, qbuf = take(0), take(0), take(0)
        if not first:
            x_out = take(0)
    w_sem = take(0)
    if not first:
        wout, wup, wdown, rp, rs, es, er, ts, tr, own_sem = (take(0) for _ in range(10))
    if not last:
        (wk, wv, wq, wvt, wqt, xk, xq, x_sem, sa, ra, sah, rah, sb, rb, sbh, rbh, sd, rd,
         sy, ry, syh, ryh, sq, rq) = (take(0) for _ in range(24))
    assert not refs

    rows, width = x_in.shape
    half = rows // 2
    cols = width // 2
    hd = width // HEADS
    scale = math.log2(math.e) / math.sqrt(hd)
    x, y, z, c = coords()
    e = 1 - c
    a0, b0 = z * e + x * c, x * e + z * c
    av = [a0] + [(a0 + 4 + k) % 4 for k in OFFS[1:]]
    bv = [b0] + [(b0 + 4 + k) % 4 for k in OFFS[1:]]
    yv = [y] + [(y + 4 + k) % 4 for k in OFFS[1:]]
    fa, fb = 4 - 3 * c, 1 + 3 * c
    partner = dev(x, y, z, e)

    def dev_a(i):
        return dev(x * e + av[i] * c, y, av[i] * e + z * c, c)

    def dev_b(i):
        return dev(bv[i] * e + x * c, y, z * e + bv[i] * c, c)

    def dev_y(i, core):
        return dev(x, yv[i], z, core)

    def nat(ka, kb):
        return av[ka] * fa + bv[kb] * fb

    def nat_partner(ka, kb):
        return bv[ka] * fb + av[kb] * fa

    started = []

    def remote(src, dst, send, recv, device):
        return pltpu.make_async_remote_copy(
            src_ref=src, dst_ref=dst, send_sem=send, recv_sem=recv, device_id=device, device_id_type=MESH)

    def go(*args):
        copy = remote(*args)
        copy.start()
        started.append(copy)

    if first:
        own = pltpu.make_async_copy(x_in, xk.at[c * 16 + z * 4 + x], x_sem)
        own.start()
    loads = []
    if not last:
        for i, dst in enumerate((wq, wk, wv)):
            src = hqkv.at[l, :, pl.ds(pl.multiple_of(i * width + c * cols, cols), cols)]
            loads.append(pltpu.make_async_copy(src, dst, w_sem.at[i]))
    if not first:
        for i, (src, dst) in enumerate(((hout, wout), (hup, wup), (hdown, wdown))):
            loads.append(pltpu.make_async_copy(src.at[l - 1], dst, w_sem.at[3 + i]))
    for load in loads:
        load.start()

    barrier = pltpu.get_barrier_semaphore()
    peers = [partner]
    if not last:
        peers += [dev_a(1), dev_a(2), dev_b(1), dev_b(2)]
    if first:
        peers += [dev_y(1, c), dev_y(2, c)]
    else:
        peers += [dev_y(i, core) for i in (1, 2, 3) for core in (0, 1)]
    for peer in peers:
        pl.semaphore_signal(barrier, inc=1, device_id=peer, device_id_type=MESH)
    pl.semaphore_wait(barrier, len(peers))

    if not first:
        def ret(i, core, src_slot):
            go(sin.at[src_slot], rs.at[y, c], ts.at[i, core], tr.at[y, c], dev_y(i, core))
            go(pin.at[src_slot], rp.at[y, c], es.at[i, core], er.at[y, c], dev_y(i, core))

        for i in (3, 1, 2):
            for core in (0, 1):
                ret(i, core, yv[i] * 2 + core)
        go(sin.at[y * 2 + e], rs.at[y, c], ts.at[0, 0], tr.at[y, c], partner)
        go(pin.at[y * 2 + e], rp.at[y, c], es.at[0, 0], er.at[y, c], partner)
        own_s = pltpu.make_async_copy(sin.at[y * 2 + c], rs.at[y, c], own_sem.at[0])
        own_p = pltpu.make_async_copy(pin.at[y * 2 + c], rp.at[y, c], own_sem.at[1])
        own_s.start()
        own_p.start()

    def project_setup():
        if last:
            return
        qbuf[...] = jnp.zeros_like(qbuf)
        vbuf[:, :, 2 * hd:, :] = jnp.ones((vbuf.shape[0], 2, vbuf.shape[2] - 2 * hd, rows), BF16)
        for load in loads[:3]:
            load.wait()
        wqt[...] = wq[...].T
        wvt[...] = wv[...].T

    if not first:
        project_setup()
        for load in loads[0 if last else 3:]:
            load.wait()
        own_s.wait()
        own_p.wait()

        def wait_in(buf, recv, i, core):
            remote(buf.at[yv[i], core], buf.at[yv[i], core], es.at[0, 0], recv.at[yv[i], core], partner).wait_recv()

        wait_in(rs, tr, 0, e)
        wait_in(rp, er, 0, e)
        for i in (1, 2, 3):
            for core in (0, 1):
                wait_in(rs, tr, i, core)
                wait_in(rp, er, i, core)
        parts = []
        for g in range(2):
            stats = [rs[yv[i], g] for i in range(4)]
            top = functools.reduce(jnp.maximum, [t[:4] for t in stats])
            share = [jnp.exp2(t[:4] - top) for t in stats]
            mass = functools.reduce(jnp.add, [f * t[4:] for f, t in zip(share, stats)])
            inverse = 1.0 / mass
            share = [f * inverse for f in share]
            for h in range(4):
                span = slice(h * hd, (h + 1) * hd)
                total = rp[yv[0], g, span].astype(F32) * share[0][h:h + 1]
                for i in (1, 2, 3):
                    total = total + rp[yv[i], g, span].astype(F32) * share[i][h:h + 1]
                parts.append(total)
        attn = jnp.concatenate(parts, axis=0).T.astype(BF16)
        mixed = jnp.dot(attn, wout[...], preferred_element_type=F32)
        hidden = layer_norm(x_in[...].astype(F32) + mixed,
                            gain[l - 1, 0:1], bias[l - 1, 0:1]).astype(BF16)
        up = gelu(jnp.dot(hidden, wup[...], preferred_element_type=F32)).astype(BF16)
        down = jnp.dot(up, wdown[...], preferred_element_type=F32)
        x_new = layer_norm(hidden.astype(F32) + down, gain[l - 1, 1:2], bias[l - 1, 1:2]).astype(BF16)
        if not last:
            xk[c * 16 + z * 4 + x] = x_new
        x_out[...] = x_new

    if not last:
        own_slot = c * 16 + z * 4 + x
        lo, hi = pl.ds(0, half), pl.ds(half, half)

        if first:
            own.wait()

        def send_b(ka):
            s = c * 16 + nat(ka, 0)
            go(xk.at[s], xk.at[s], sb.at[ka, 0], rb.at[ka, 0], dev_b(2))
            go(xk.at[s], xk.at[s], sb.at[ka, 1], rb.at[ka, 1], dev_b(1))

        def to_partner(ka, kb):
            n = nat(ka, kb)
            go(xk.at[c * 16 + n], xk.at[c * 16 + n], sd.at[n], rd.at[n], partner)

        def await_k(s, rows_, recv):
            ref = xk.at[s] if rows_ is None else xk.at[s, rows_]
            remote(ref, ref, sd.at[0], recv, partner).wait_recv()

        go(xk.at[own_slot], xk.at[own_slot], sa.at[0], ra.at[0], dev_a(2))
        go(xk.at[own_slot], xk.at[own_slot], sa.at[1], ra.at[1], dev_a(1))
        send_b(0)
        go(xk.at[own_slot], xq.at[c, y], sy.at[0], ry.at[0], dev_y(2, c))
        go(xk.at[own_slot], xq.at[c, y], sy.at[1], ry.at[1], dev_y(1, c))
        to_partner(0, 0)
        if first:
            project_setup()

        def project_kv(s):
            xs = xk[s]
            k = jnp.dot(xs, wk[...], preferred_element_type=F32)
            kbuf[s] = k.astype(BF16)
            v = lax.dot_general(wvt[...], xs, (((1,), (1,)), ((), ())), preferred_element_type=F32).astype(BF16)
            vbuf[s, 0, :2 * hd] = v[:2 * hd]
            vbuf[s, 1, :2 * hd] = v[2 * hd:]

        def project_q(q, xs):
            t = lax.dot_general(wqt[...], xs, (((1,), (1,)), ((), ())), preferred_element_type=F32)
            t = (t * scale).astype(BF16)
            for h in range(2):
                base = h * 2 * hd
                qbuf[q, h, :hd, :rows] = t[base:base + hd]
                qbuf[q, h, hd:, rows:] = t[base + hd:base + 2 * hd]

        def handle(ka, kb):
            s = c * 16 + nat(ka, kb)
            if kb == 0:
                if ka == 0:
                    return
                if ka < 3:
                    await_k(s, None, ra.at[ka - 1])
                    part = lo if ka == 1 else hi
                    go(xk.at[s, part], xk.at[s, part], sah.at[ka - 1], rah.at[ka - 1], dev_a(3 - ka))
                else:
                    await_k(s, lo, rah.at[0])
                    await_k(s, hi, rah.at[1])
                send_b(ka)
            elif kb < 3:
                await_k(s, None, rb.at[ka, kb - 1])
                part = lo if kb == 1 else hi
                go(xk.at[s, part], xk.at[s, part], sbh.at[ka, kb - 1], rbh.at[ka, kb - 1], dev_b(3 - kb))
            else:
                await_k(s, lo, rbh.at[ka, 0])
                await_k(s, hi, rbh.at[ka, 1])
            to_partner(ka, kb)

        def handle_y(i):
            if i < 3:
                ref = xq.at[c, yv[i]]
                remote(ref, ref, sy.at[0], ry.at[i - 1], partner).wait_recv()
                part = lo if i == 1 else hi
                ref = xq.at[c, yv[i], part]
                go(ref, ref, syh.at[i - 1], ryh.at[i - 1], dev_y(3 - i, c))
            else:
                for j, part in enumerate((lo, hi)):
                    ref = xq.at[c, yv[3], part]
                    remote(ref, ref, sy.at[0], ryh.at[j], partner).wait_recv()
            ref = xq.at[c, yv[i]]
            go(ref, ref, sq.at[i - 1], rq.at[i - 1], partner)

        def finish(ka, kb):
            n, m = nat(ka, kb), nat_partner(ka, kb)
            s, t = c * 16 + n, e * 16 + m
            await_k(t, None, rd.at[m])

            @pl.loop(0, 2)
            def _(i):
                project_kv(s + i * (t - s))

        def finish_y(i):
            if i == 0:
                project_q(y * 2 + c, xk[own_slot])
                project_q(y * 2 + e, xk[e * 16 + z * 4 + x])
                return
            ref = xq.at[e, yv[i]]
            remote(ref, ref, sq.at[0], rq.at[i - 1], partner).wait_recv()

            @pl.loop(0, 2)
            def _(core):
                project_q(yv[i] * 2 + core, xq[core, yv[i]])

        todo = []
        ypos = {2: (1,), 4: (2,), 7: (3,)}
        for pos, (ka, kb) in enumerate(ORDER):
            handle(ka, kb)
            todo.append(functools.partial(finish, ka, kb))
            if pos == 0:
                todo.append(functools.partial(finish_y, 0))
            for i in ypos.get(pos, ()):
                handle_y(i)
                todo.append(functools.partial(finish_y, i))
            while len(todo) > 2:
                todo.pop(0)()
        for f in todo:
            f()

    for copy in started:
        copy.wait_send()


def attend(mask, kbuf, vbuf, qbuf, pout, sout, smask, pairs, acc, top, den, sem):
    n_q, n_k, rows = qbuf.shape[0], kbuf.shape[0], kbuf.shape[1]
    hd = qbuf.shape[2] // 2
    x, y, z, c = coords()
    row = lax.axis_index("row")
    load = pltpu.make_async_copy(mask.at[pl.ds(row * 16, 16)], smask, sem)
    load.start()
    acc[...] = jnp.zeros_like(acc)
    den[...] = jnp.zeros_like(den)
    top[...] = jnp.full_like(top, FLOOR)
    load.wait()

    def scan(q, n):
        at = (q // 2) * 4 + (x % 2) * 2 + q % 2
        for s in range(n_k):
            core, zz, xx = s // 16, (s % 16) // 4, s % 4
            kid = (zz * 2 + xx // 2) * 16 + y * 4 + (xx % 2) * 2 + core
            pairs[n] = q * n_k + s
            n = n + jnp.where(smask[at, kid] > 0, 1, 0)
        return n

    n = lax.fori_loop(0, n_q, scan, 0)
    for i in range(UNROLL - 1):
        pairs[n + i] = n_q * n_k

    @pl.loop(0, (n + UNROLL - 1) // UNROLL)
    def _(it):
        for u in range(UNROLL):
            code = pairs[it * UNROLL + u]
            q, k = code // n_k, code % n_k
            src = jnp.minimum(q, n_q - 1)
            for h in range(2):
                s = jnp.dot(kbuf[k, :, h * 2 * hd:(h + 1) * 2 * hd], qbuf[src, h], preferred_element_type=F32)
                old = top[q, h]
                new = jnp.maximum(old, jnp.max(s, axis=0, keepdims=True))
                p = jnp.exp2(s - new).astype(BF16)
                o = jnp.dot(vbuf[k, h], p, preferred_element_type=F32)
                alpha = jnp.exp2(old - new)
                top[q, h] = new
                den[q, h] = den[q, h] * alpha + o[2 * hd:2 * hd + 1]
                for g in range(2):
                    lanes = slice(g * rows, (g + 1) * rows)
                    span = slice((2 * h + g) * hd, (2 * h + g + 1) * hd)
                    acc[q, span] = acc[q, span] * alpha[:, lanes] + o[g * hd:(g + 1) * hd, lanes]

    for q in range(n_q):
        pout[q] = acc[q].astype(BF16)
        for h in range(2):
            for g in range(2):
                lanes = slice(g * rows, (g + 1) * rows)
                sout[q, 2 * h + g:2 * h + g + 1] = top[q, h, :, lanes]
                sout[q, 4 + 2 * h + g:5 + 2 * h + g] = den[q, h, :, lanes]


def solution(mesh):
    def per_device(x, mask, wqkv, wout, wup, wdown, gain, bias):
        rows, width = x.shape
        layers = wqkv.shape[0]
        cols = width // 2
        ff = wup.shape[2]
        hd = width // HEADS
        n_q, n_k = 8, 32
        vmem, any_ = pl.BlockSpec(memory_space=pltpu.VMEM), pl.BlockSpec(memory_space=pl.ANY)
        dma = pltpu.SemaphoreType.DMA
        shape = jax.ShapeDtypeStruct
        proj = [shape((n_k, rows, cols), BF16), shape((n_k, 2, 2 * hd + 16, rows), BF16),
                shape((n_q, 2, 2 * hd, 2 * rows), BF16)]

        def call_exchange(l, x, part):
            first, last = l == 0, l == layers
            ins, specs, outs = [x], [any_ if first else vmem], []
            if not first:
                ins += part
                specs += [vmem, vmem]
            if not last:
                ins.append(wqkv)
                specs.append(any_)
            if not first:
                ins += [wout, wup, wdown, gain, bias]
                specs += [any_] * 3 + [vmem] * 2
            if not last:
                outs += proj
            if not first:
                outs.append(shape((rows, width), BF16))
            scratch = [dma((6,))]
            if not first:
                scratch += [pltpu.VMEM((width, width), BF16), pltpu.VMEM((width, ff), BF16),
                            pltpu.VMEM((ff, width), BF16),
                            pltpu.VMEM((4, 2, cols, rows), BF16), pltpu.VMEM((4, 2, 8, rows), F32),
                            dma((4, 2)), dma((4, 2)), dma((4, 2)), dma((4, 2)), dma((2,))]
            if not last:
                scratch += [pltpu.VMEM((width, cols), BF16)] * 3 + [pltpu.VMEM((cols, width), BF16)] * 2
                scratch += [pltpu.VMEM((n_k, rows, width), BF16), pltpu.VMEM((2, 4, rows, width), BF16), dma]
                scratch += [dma((2,))] * 4 + [dma((4, 2))] * 4 + [dma((16,))] * 2
                scratch += [dma((2,))] * 4 + [dma((3,))] * 2
            return pl.pallas_call(
                functools.partial(exchange, l, first, last),
                out_shape=outs, in_specs=specs, out_specs=[vmem] * len(outs), scratch_shapes=scratch,
                compiler_params=pltpu.CompilerParams(
                    collective_id=l, has_side_effects=True, vmem_limit_bytes=28 * 1024 * 1024),
            )(*ins)

        def call_attend(projected):
            return pl.pallas_call(
                attend,
                out_shape=[shape((n_q, cols, rows), BF16), shape((n_q, 8, rows), F32)],
                in_specs=[any_, vmem, vmem, vmem], out_specs=[vmem, vmem],
                scratch_shapes=[
                    pltpu.SMEM((16, 128), jnp.int32), pltpu.SMEM((n_q * n_k + UNROLL,), jnp.int32),
                    pltpu.VMEM((n_q + 1, cols, rows), F32), pltpu.VMEM((n_q + 1, 2, 1, 2 * rows), F32),
                    pltpu.VMEM((n_q + 1, 2, 1, 2 * rows), F32), dma],
                compiler_params=pltpu.CompilerParams(vmem_limit_bytes=28 * 1024 * 1024),
            )(mask, *projected)

        projected = call_exchange(0, x, None)
        for l in range(1, layers):
            *projected, x = call_exchange(l, x, call_attend(projected))
        return call_exchange(layers, x, call_attend(projected))[0]

    placed = (P(("row", "col"), None), P(), P(), P(), P(), P(), P(), P())
    return jax.shard_map(
        per_device, mesh=mesh, in_specs=placed, out_specs=P(("row", "col"), None), check_vma=False
    )
```

```python
import functools
import math

import jax
import jax.numpy as jnp
from jax import lax
from jax.experimental import pallas as pl
from jax.experimental.pallas import tpu as pltpu
from jax.sharding import PartitionSpec as P

HEADS = 8
F32, BF16 = jnp.float32, jnp.bfloat16
FLOOR = -1e30
MESH = pl.DeviceIdType.MESH
OFFS = (0, -1, 1, 2)
GROUP, AHEAD = 4, 4


def layer_norm(values, gain, bias):
    center = values - jnp.mean(values, axis=-1, keepdims=True)
    spread = jnp.mean(center * center, axis=-1, keepdims=True)
    return center * lax.rsqrt(spread + 1e-05) * gain + bias


def gelu(v):
    inner = math.sqrt(2.0 / math.pi) * (v + 0.044715 * (v * v * v))
    return v * (0.5 * (1.0 + jnp.tanh(inner)))


def coords():
    row, col = lax.axis_index("row"), lax.axis_index("col")
    return (row % 2) * 2 + (col // 2) % 2, col // 4, row // 2, col % 2


def dev(x, y, z, c):
    return {"row": z * 2 + x // 2, "col": y * 4 + (x % 2) * 2 + c}


def exchange(l, first, last, *refs):
    refs = list(refs)
    take = refs.pop
    x_in = take(0)
    if not first:
        pin, sin = take(0), take(0)
    hqkv = None if last else take(0)
    if not first:
        hout, hup, hdown, gain, bias = (take(0) for _ in range(5))
    if last:
        x_out = take(0)
    else:
        kbuf, vbuf, qbuf = take(0), take(0), take(0)
        if not first:
            x_out = take(0)
    w_sem, snd = take(0), take(0)
    if not first:
        wout, wup, wdown, rp, rs, er, tr, own_sem = (take(0) for _ in range(8))
    if not last:
        wk, wv, wq, wvt, wqt, xk, xq, x_sem, ra, rb, rd, ry, rq = (take(0) for _ in range(13))
    assert not refs

    rows, width = x_in.shape
    half = rows // 2
    cols = width // 2
    hd = width // HEADS
    scale = math.log2(math.e) / math.sqrt(hd)
    x, y, z, c = coords()
    e = 1 - c
    a0, b0 = z * e + x * c, x * e + z * c
    av = [a0] + [(a0 + 4 + k) % 4 for k in OFFS[1:]]
    bv = [b0] + [(b0 + 4 + k) % 4 for k in OFFS[1:]]
    yv = [y] + [(y + 4 + k) % 4 for k in OFFS[1:]]
    fa, fb = 4 - 3 * c, 1 + 3 * c
    partner = dev(x, y, z, e)

    def dev_a(i):
        return dev(x * e + av[i] * c, y, av[i] * e + z * c, c)

    def dev_b(i):
        return dev(bv[i] * e + x * c, y, z * e + bv[i] * c, c)

    def dev_y(i, core):
        return dev(x, yv[i], z, core)

    def nat(ka, kb):
        return av[ka] * fa + bv[kb] * fb

    def nat_partner(ka, kb):
        return bv[ka] * fb + av[kb] * fa

    started = []

    def remote(src, dst, send, recv, device):
        return pltpu.make_async_remote_copy(
            src_ref=src, dst_ref=dst, send_sem=send, recv_sem=recv, device_id=device, device_id_type=MESH)

    def go(src, dst, recv, device):
        copy = remote(src, dst, snd.at[len(started)], recv, device)
        copy.start()
        started.append(copy)

    if first:
        own = pltpu.make_async_copy(x_in, xk.at[c * 16 + z * 4 + x], x_sem)
        own.start()
    loads = []
    if not last:
        for i, dst in enumerate((wq, wk, wv)):
            src = hqkv.at[l, :, pl.ds(pl.multiple_of(i * width + c * cols, cols), cols)]
            loads.append(pltpu.make_async_copy(src, dst, w_sem.at[i]))
    if not first:
        for i, (src, dst) in enumerate(((hout, wout), (hup, wup), (hdown, wdown))):
            loads.append(pltpu.make_async_copy(src.at[l - 1], dst, w_sem.at[3 + i]))
    for load in loads:
        load.start()

    barrier = pltpu.get_barrier_semaphore()
    peers = [partner]
    if not last:
        peers += [dev_a(1), dev_a(2), dev_b(1), dev_b(2)]
    if first:
        peers += [dev_y(1, c), dev_y(2, c)]
    else:
        peers += [dev_y(i, core) for i in (1, 2, 3) for core in (0, 1)]
    for peer in peers:
        pl.semaphore_signal(barrier, inc=1, device_id=peer, device_id_type=MESH)
    pl.semaphore_wait(barrier, len(peers))

    if not first:
        def ret(i, core, src_slot):
            go(sin.at[src_slot], rs.at[y, c], tr.at[y, c], dev_y(i, core))
            go(pin.at[src_slot], rp.at[y, c], er.at[y, c], dev_y(i, core))

        for i in (3, 1, 2):
            for core in (0, 1):
                ret(i, core, yv[i] * 2 + core)
        go(sin.at[y * 2 + e], rs.at[y, c], tr.at[y, c], partner)
        go(pin.at[y * 2 + e], rp.at[y, c], er.at[y, c], partner)
        own_s = pltpu.make_async_copy(sin.at[y * 2 + c], rs.at[y, c], own_sem.at[0])
        own_p = pltpu.make_async_copy(pin.at[y * 2 + c], rp.at[y, c], own_sem.at[1])
        own_s.start()
        own_p.start()

    def project_setup():
        if last:
            return
        qbuf[...] = jnp.zeros_like(qbuf)
        n_k = kbuf.shape[0]
        vbuf[:n_k, :, 2 * hd:, :] = jnp.ones((n_k, 2, vbuf.shape[2] - 2 * hd, rows), BF16)
        vbuf[n_k] = jnp.zeros(vbuf.shape[1:], BF16)
        for load in loads[:3]:
            load.wait()
        wqt[...] = wq[...].T
        wvt[...] = wv[...].T

    if not first:
        project_setup()
        for load in loads[0 if last else 3:]:
            load.wait()
        own_s.wait()
        own_p.wait()

        def wait_in(buf, recv, i, core):
            remote(buf.at[yv[i], core], buf.at[yv[i], core], snd.at[0], recv.at[yv[i], core], partner).wait_recv()

        wait_in(rs, tr, 0, e)
        wait_in(rp, er, 0, e)
        for i in (1, 2, 3):
            for core in (0, 1):
                wait_in(rs, tr, i, core)
                wait_in(rp, er, i, core)
        parts = []
        for g in range(2):
            stats = [rs[yv[i], g] for i in range(4)]
            top = functools.reduce(jnp.maximum, [t[:4] for t in stats])
            share = [jnp.exp2(t[:4] - top) for t in stats]
            mass = functools.reduce(jnp.add, [f * t[4:] for f, t in zip(share, stats)])
            inverse = 1.0 / mass
            share = [f * inverse for f in share]
            for h in range(4):
                span = slice(h * hd, (h + 1) * hd)
                total = rp[yv[0], g, span].astype(F32) * share[0][h:h + 1]
                for i in (1, 2, 3):
                    total = total + rp[yv[i], g, span].astype(F32) * share[i][h:h + 1]
                parts.append(total)
        attn = jnp.concatenate(parts, axis=0).T.astype(BF16)
        mixed = jnp.dot(attn, wout[...], preferred_element_type=F32)
        hidden = layer_norm(x_in[...].astype(F32) + mixed,
                            gain[l - 1, 0:1], bias[l - 1, 0:1]).astype(BF16)
        up = gelu(jnp.dot(hidden, wup[...], preferred_element_type=F32)).astype(BF16)
        down = jnp.dot(up, wdown[...], preferred_element_type=F32)
        x_new = layer_norm(hidden.astype(F32) + down, gain[l - 1, 1:2], bias[l - 1, 1:2]).astype(BF16)
        if not last:
            xk[c * 16 + z * 4 + x] = x_new
        x_out[...] = x_new

    if not last:
        own_slot = c * 16 + z * 4 + x
        if first:
            own.wait()

        def part(ref, h):
            return ref if h is None else ref.at[pl.ds(h * half, half)]

        def arrived(ref, recv):
            remote(ref, ref, snd.at[0], recv, partner).wait_recv()

        def send_a(ka, h, up):
            ref = part(xk.at[c * 16 + nat(ka, 0)], h)
            to = (1 if up else 2) if ka == 0 else 3
            go(ref, ref, ra.at[to - 1, h], dev_a(2 if up else 1))

        def wait_a(ka, h):
            arrived(part(xk.at[c * 16 + nat(ka, 0)], h), ra.at[ka - 1, h])

        def send_b(ka, kb, h, up):
            ref = part(xk.at[c * 16 + nat(ka, kb)], h)
            to = (1 if up else 2) if kb == 0 else 3
            go(ref, ref, rb.at[ka, to - 1, h], dev_b(2 if up else 1))

        def wait_b(ka, kb, h):
            arrived(part(xk.at[c * 16 + nat(ka, kb)], h), rb.at[ka, kb - 1, h])

        def send_y(i, h, up):
            ref = part(xk.at[own_slot] if i == 0 else xq.at[c, yv[i]], h)
            to = (1 if up else 2) if i == 0 else 3
            go(ref, part(xq.at[c, yv[i]], h), ry.at[to - 1, h], dev_y(2 if up else 1, c))

        def wait_y(i, h):
            arrived(part(xq.at[c, yv[i]], h), ry.at[i - 1, h])

        def share(ka, kb):
            n = nat(ka, kb)
            go(xk.at[c * 16 + n], xk.at[c * 16 + n], rd.at[n], partner)

        def share_y(i):
            ref = xq.at[c, yv[i]]
            go(ref, ref, rq.at[i - 1], partner)

        def project_kv(s, t):
            xs = jnp.concatenate([xk[s], xk[t]], axis=0)
            k = jnp.dot(xs, wk[...], preferred_element_type=F32).astype(BF16)
            v = lax.dot_general(wvt[...], xs, (((1,), (1,)), ((), ())), preferred_element_type=F32).astype(BF16)
            for i, to in enumerate((s, t)):
                span = slice(i * rows, (i + 1) * rows)
                kbuf[to] = k[span]
                vbuf[to, 0, :2 * hd] = v[:2 * hd, span]
                vbuf[to, 1, :2 * hd] = v[2 * hd:, span]

        def project_q(q, xs):
            t = lax.dot_general(wqt[...], xs, (((1,), (1,)), ((), ())), preferred_element_type=F32)
            t = (t * scale).astype(BF16)
            for h in range(2):
                base = h * 2 * hd
                qbuf[q, h, :hd, :rows] = t[base:base + hd]
                qbuf[q, h, hd:, rows:] = t[base + hd:base + 2 * hd]

        def finish(*blocks):
            for ka, kb in blocks:
                n, m = nat(ka, kb), nat_partner(ka, kb)
                s, t = c * 16 + n, e * 16 + m
                arrived(xk.at[t], rd.at[m])
                project_kv(s, t)

        def finish_y(*which):
            for i in which:
                if i == 0:
                    project_q(y * 2 + c, xk[own_slot])
                    project_q(y * 2 + e, xk[e * 16 + z * 4 + x])
                    continue
                arrived(xq.at[e, yv[i]], rq.at[i - 1])

                @pl.loop(0, 2)
                def _(core):
                    project_q(yv[i] * 2 + core, xq[core, yv[i]])

        for h in (0, 1):
            send_a(0, h, True)
            send_a(0, 1 - h, False)
            send_b(0, 0, h, True)
            send_b(0, 0, 1 - h, False)
            send_y(0, h, True)
            send_y(0, 1 - h, False)
        share(0, 0)
        if first:
            project_setup()
        finish((0, 0))
        finish_y(0)
        wait_a(1, 0)
        send_a(1, 0, True)
        send_b(1, 0, 0, True)
        wait_a(2, 1)
        send_a(2, 1, False)
        send_b(2, 0, 1, False)
        wait_b(0, 1, 0)
        send_b(0, 1, 0, True)
        wait_b(0, 2, 1)
        send_b(0, 2, 1, False)
        wait_y(1, 0)
        send_y(1, 0, True)
        wait_y(2, 1)
        send_y(2, 1, False)
        wait_a(1, 1)
        send_b(1, 0, 1, False)
        wait_a(2, 0)
        send_b(2, 0, 0, True)
        send_b(1, 0, 1, True)
        send_b(1, 0, 0, False)
        send_b(2, 0, 0, False)
        send_b(2, 0, 1, True)
        share(1, 0)
        share(2, 0)
        wait_b(0, 1, 1)
        share(0, 1)
        wait_b(0, 2, 0)
        share(0, 2)
        wait_y(1, 1)
        share_y(1)
        wait_y(2, 0)
        share_y(2)
        finish((1, 0))
        wait_a(3, 0)
        send_b(3, 0, 0, True)
        wait_a(3, 1)
        send_b(3, 0, 1, False)
        send_b(3, 0, 1, True)
        send_b(3, 0, 0, False)
        share(3, 0)
        finish((2, 0), (0, 1))
        for ka in (1, 2):
            wait_b(ka, 1, 0)
            send_b(ka, 1, 0, True)
            wait_b(ka, 2, 1)
            send_b(ka, 2, 1, False)
        wait_b(0, 3, 0)
        wait_b(0, 3, 1)
        share(0, 3)
        finish((0, 2))
        finish_y(1, 2)
        for ka in (1, 2):
            wait_b(ka, 1, 1)
            share(ka, 1)
            wait_b(ka, 2, 0)
            share(ka, 2)
        wait_y(3, 0)
        wait_y(3, 1)
        share_y(3)
        finish((3, 0))
        wait_b(3, 1, 0)
        send_b(3, 1, 0, True)
        wait_b(3, 2, 1)
        send_b(3, 2, 1, False)
        finish((0, 3), (1, 1))
        for ka in (1, 2):
            wait_b(ka, 3, 0)
            wait_b(ka, 3, 1)
            share(ka, 3)
        wait_b(3, 1, 1)
        share(3, 1)
        wait_b(3, 2, 0)
        share(3, 2)
        finish((1, 2), (2, 1), (2, 2))
        finish_y(3)
        finish((1, 3), (2, 3))
        wait_b(3, 3, 0)
        wait_b(3, 3, 1)
        share(3, 3)
        finish((3, 1), (3, 2), (3, 3))

    for copy in started:
        copy.wait_send()


def attend(mask, kbuf, vbuf, qbuf, pout, sout, smask, pairs, sbuf, peak, acc, top, den, sem):
    n_q, n_k, rows = qbuf.shape[0], kbuf.shape[0], kbuf.shape[1]
    hd = qbuf.shape[2] // 2
    x, y, z, c = coords()
    row = lax.axis_index("row")
    load = pltpu.make_async_copy(mask.at[pl.ds(row * 16, 16)], smask, sem)
    load.start()
    acc[...] = jnp.zeros_like(acc)
    den[...] = jnp.zeros_like(den)
    top[...] = jnp.full_like(top, FLOOR)
    load.wait()

    def scan(q, n):
        at = (q // 2) * 4 + (x % 2) * 2 + q % 2
        base = q * 4096
        for s in range(n_k):
            core, zz, xx = s // 16, (s % 16) // 4, s % 4
            kid = (zz * 2 + xx // 2) * 16 + y * 4 + (xx % 2) * 2 + core
            pairs[n] = base + (s * 64 + s)
            n = n + smask[at, kid]
        before = pairs[jnp.maximum(n - 1, 0)]
        pairs[n] = (before // 64) * 64 + n_k
        return n + n % 2

    n = lax.fori_loop(0, n_q, scan, 0)
    for i in range(4 * GROUP):
        pairs[n + i] = n_q * 4096 + n_k

    units = 2 * GROUP

    def scores(it, i):
        d, h = i // 2, i % 2
        code = [pairs[(it * GROUP + d) * 2 + j] for j in range(2)]
        q = jnp.minimum(code[0] // 4096, n_q - 1)
        best = []
        for j in range(2):
            k = (code[j] // 64) % 64
            s = jnp.dot(kbuf[k, :, h * 2 * hd:(h + 1) * 2 * hd], qbuf[q, h], preferred_element_type=F32)
            sbuf[i, j * rows:(j + 1) * rows] = s
            best.append(jnp.max(s, axis=0, keepdims=True))
        peak[i] = jnp.maximum(*best)

    def values(it, i):
        d, h = i // 2, i % 2
        code = [pairs[(it * GROUP + d) * 2 + j] for j in range(2)]
        q = code[0] // 4096
        old = top[q, h]
        new = jnp.maximum(old, peak[i])
        p = jnp.exp2(sbuf[i] - new).astype(BF16)
        v = jnp.concatenate([vbuf[code[j] % 64, h] for j in range(2)], axis=1)
        o = jnp.dot(v, p, preferred_element_type=F32)
        alpha = jnp.exp2(old - new)
        top[q, h] = new
        den[q, h] = den[q, h] * alpha + o[2 * hd:2 * hd + 1]
        for g in range(2):
            lanes = slice(g * rows, (g + 1) * rows)
            span = slice((2 * h + g) * hd, (2 * h + g + 1) * hd)
            acc[q, span] = acc[q, span] * alpha[:, lanes] + o[g * hd:(g + 1) * hd, lanes]

    for i in range(AHEAD):
        scores(0, i)

    @pl.loop(0, (n + 2 * GROUP - 1) // (2 * GROUP))
    def _(it):
        for i in range(units):
            ahead = i + AHEAD
            scores(it + ahead // units, ahead % units)
            values(it, i)

    for q in range(n_q):
        pout[q] = acc[q].astype(BF16)
        for h in range(2):
            for g in range(2):
                lanes = slice(g * rows, (g + 1) * rows)
                sout[q, 2 * h + g:2 * h + g + 1] = top[q, h, :, lanes]
                sout[q, 4 + 2 * h + g:5 + 2 * h + g] = den[q, h, :, lanes]


def solution(mesh):
    def per_device(x, mask, wqkv, wout, wup, wdown, gain, bias):
        rows, width = x.shape
        layers = wqkv.shape[0]
        cols = width // 2
        ff = wup.shape[2]
        hd = width // HEADS
        n_q, n_k = 8, 32
        vmem, any_ = pl.BlockSpec(memory_space=pltpu.VMEM), pl.BlockSpec(memory_space=pltpu.HBM)
        dma = pltpu.SemaphoreType.DMA
        shape = jax.ShapeDtypeStruct
        proj = [shape((n_k, rows, cols), BF16), shape((n_k + 1, 2, 2 * hd + 16, rows), BF16),
                shape((n_q, 2, 2 * hd, 2 * rows), BF16)]

        def call_exchange(l, x, part):
            first, last = l == 0, l == layers
            ins, specs, outs = [x], [any_ if first else vmem], []
            if not first:
                ins += part
                specs += [vmem, vmem]
            if not last:
                ins.append(wqkv)
                specs.append(any_)
            if not first:
                ins += [wout, wup, wdown, gain, bias]
                specs += [any_] * 3 + [vmem] * 2
            if not last:
                outs += proj
            if not first:
                outs.append(shape((rows, width), BF16))
            scratch = [dma((6,)), dma((96,))]
            if not first:
                scratch += [pltpu.VMEM((width, width), BF16), pltpu.VMEM((width, ff), BF16),
                            pltpu.VMEM((ff, width), BF16),
                            pltpu.VMEM((4, 2, cols, rows), BF16), pltpu.VMEM((4, 2, 8, rows), F32),
                            dma((4, 2)), dma((4, 2)), dma((2,))]
            if not last:
                scratch += [pltpu.VMEM((width, cols), BF16)] * 3 + [pltpu.VMEM((cols, width), BF16)] * 2
                scratch += [pltpu.VMEM((n_k, rows, width), BF16), pltpu.VMEM((2, 4, rows, width), BF16), dma]
                scratch += [dma((3, 2)), dma((4, 3, 2)), dma((16,)), dma((3, 2)), dma((3,))]
            return pl.pallas_call(
                functools.partial(exchange, l, first, last),
                out_shape=outs, in_specs=specs, out_specs=[vmem] * len(outs), scratch_shapes=scratch,
                compiler_params=pltpu.CompilerParams(
                    collective_id=l, has_side_effects=True, vmem_limit_bytes=28 * 1024 * 1024),
            )(*ins)

        def call_attend(projected):
            return pl.pallas_call(
                attend,
                out_shape=[shape((n_q, cols, rows), BF16), shape((n_q, 8, rows), F32)],
                in_specs=[any_, vmem, vmem, vmem], out_specs=[vmem, vmem],
                scratch_shapes=[
                    pltpu.SMEM((16, 128), jnp.int32), pltpu.SMEM((n_q * n_k + 4 * GROUP + 1,), jnp.int32),
                    pltpu.VMEM((2 * GROUP, 2 * rows, 2 * rows), F32), pltpu.VMEM((2 * GROUP, 1, 2 * rows), F32),
                    pltpu.VMEM((n_q + 1, cols, rows), F32), pltpu.VMEM((n_q + 1, 2, 1, 2 * rows), F32),
                    pltpu.VMEM((n_q + 1, 2, 1, 2 * rows), F32), dma],
                compiler_params=pltpu.CompilerParams(vmem_limit_bytes=28 * 1024 * 1024),
            )(mask, *projected)

        x = pltpu.with_memory_space_constraint(x, pltpu.HBM)
        wqkv = pltpu.with_memory_space_constraint(wqkv, pltpu.HBM)
        projected = call_exchange(0, x, None)
        for l in range(1, layers):
            *projected, x = call_exchange(l, x, call_attend(projected))
        return call_exchange(layers, x, call_attend(projected))[0]

    placed = (P(("row", "col"), None), P(), P(), P(), P(), P(), P(), P())
    return jax.shard_map(
        per_device, mesh=mesh, in_specs=placed, out_specs=P(("row", "col"), None), check_vma=False
    )
```

```python
import functools
import math

import jax
import jax.numpy as jnp
from jax import lax
from jax.experimental import pallas as pl
from jax.experimental.pallas import tpu as pltpu
from jax.sharding import PartitionSpec as P

HEADS = 8
F32, BF16 = jnp.float32, jnp.bfloat16
FLOOR = -1e30
MESH = pl.DeviceIdType.MESH
OFFS = (0, -1, 1, 2)
GROUP, AHEAD = 4, 4
GROUPS = (((0, 0),), ((1, 0),), ((2, 0), (0, 1)), ((0, 2),), ((3, 0),), ((0, 3), (1, 1)),
          ((1, 2), (2, 1), (2, 2)), ((1, 3), (2, 3)), ((3, 1), (3, 2)), ((3, 3),))
GROUP_OF = {block: i for i, group in enumerate(GROUPS) for block in group}


def layer_norm(values, gain, bias):
    center = values - jnp.mean(values, axis=-1, keepdims=True)
    spread = jnp.mean(center * center, axis=-1, keepdims=True)
    return center * lax.rsqrt(spread + 1e-05) * gain + bias


def gelu(v):
    inner = math.sqrt(2.0 / math.pi) * (v + 0.044715 * (v * v * v))
    return v * (0.5 * (1.0 + jnp.tanh(inner)))


def coords():
    row, col = lax.axis_index("row"), lax.axis_index("col")
    return (row % 2) * 2 + (col // 2) % 2, col // 4, row // 2, col % 2


def dev(x, y, z, c):
    return {"row": z * 2 + x // 2, "col": y * 4 + (x % 2) * 2 + c}


def exchange(l, first, last, *refs):
    refs = list(refs)
    take = refs.pop
    x_in = take(0)
    if first:
        mask = take(0)
    else:
        pin, sin = take(0), take(0)
    hqkv = None if last else take(0)
    if not first:
        hout, hup, hdown, gain, bias = (take(0) for _ in range(5))
    if last:
        x_out = take(0)
    else:
        kbuf, vbuf, qbuf = take(0), take(0), take(0)
        if first:
            listed = take(0)
        else:
            x_out = take(0)
    w_sem, snd = take(0), take(0)
    if first:
        masked, m_sem = take(0), take(0)
    if not first:
        wout, wup, wdown, rp, rs, er, tr, own_sem = (take(0) for _ in range(8))
    if not last:
        wk, wv, wq, wvt, wqt, xk, xq, x_sem, ra, rb, rd, ry, rq = (take(0) for _ in range(13))
    assert not refs

    rows, width = x_in.shape
    half = rows // 2
    cols = width // 2
    hd = width // HEADS
    scale = math.log2(math.e) / math.sqrt(hd)
    x, y, z, c = coords()
    e = 1 - c
    a0, b0 = z * e + x * c, x * e + z * c
    av = [a0] + [(a0 + 4 + k) % 4 for k in OFFS[1:]]
    bv = [b0] + [(b0 + 4 + k) % 4 for k in OFFS[1:]]
    yv = [y] + [(y + 4 + k) % 4 for k in OFFS[1:]]
    fa, fb = 4 - 3 * c, 1 + 3 * c
    partner = dev(x, y, z, e)

    def dev_a(i):
        return dev(x * e + av[i] * c, y, av[i] * e + z * c, c)

    def dev_b(i):
        return dev(bv[i] * e + x * c, y, z * e + bv[i] * c, c)

    def dev_y(i, core):
        return dev(x, yv[i], z, core)

    def nat(ka, kb):
        return av[ka] * fa + bv[kb] * fb

    def nat_partner(ka, kb):
        return bv[ka] * fb + av[kb] * fa


    def remote(src, dst, send, recv, device):
        return pltpu.make_async_remote_copy(
            src_ref=src, dst_ref=dst, send_sem=send, recv_sem=recv, device_id=device, device_id_type=MESH)

    def go(kind, src, dst, recv, device):
        remote(src, dst, snd.at[kind], recv, device).start()

    if first:
        own = pltpu.make_async_copy(x_in, xk.at[c * 16 + z * 4 + x], x_sem)
        own.start()
        own_mask = pltpu.make_async_copy(mask, masked, m_sem)
        own_mask.start()
    loads = []
    if not last:
        for i, dst in enumerate((wq, wk, wv)):
            src = hqkv.at[l, :, pl.ds(pl.multiple_of(i * width + c * cols, cols), cols)]
            loads.append(pltpu.make_async_copy(src, dst, w_sem.at[i]))
    if not first:
        for i, (src, dst) in enumerate(((hout, wout), (hup, wup), (hdown, wdown))):
            loads.append(pltpu.make_async_copy(src.at[l - 1], dst, w_sem.at[3 + i]))
    for load in loads:
        load.start()

    barrier = pltpu.get_barrier_semaphore()
    peers = [partner]
    if not last:
        peers += [dev_a(1), dev_a(2), dev_b(1), dev_b(2)]
    if first:
        peers += [dev_y(1, c), dev_y(2, c)]
    else:
        peers += [dev_y(i, core) for i in (1, 2, 3) for core in (0, 1)]
    for peer in peers:
        pl.semaphore_signal(barrier, inc=1, device_id=peer, device_id_type=MESH)
    pl.semaphore_wait(barrier, len(peers))

    if not first:
        def ret(i, core):
            src, to = yv[i] * 2 + core, y * 2 + c
            go(0, sin.at[src], rs.at[to], tr, dev_y(i, core))
            go(1, pin.at[src], rp.at[to], er, dev_y(i, core))

        for i in (3, 1, 2):
            for core in (0, 1):
                ret(i, core)
        ret(0, e)
        own_s = pltpu.make_async_copy(sin.at[y * 2 + c], rs.at[y * 2 + c], own_sem.at[0])
        own_p = pltpu.make_async_copy(pin.at[y * 2 + c], rp.at[y * 2 + c], own_sem.at[1])
        own_s.start()
        own_p.start()

    def project_setup():
        if last:
            return
        qbuf[...] = jnp.zeros_like(qbuf)
        n_k = kbuf.shape[0]
        vbuf[:n_k, :, 2 * hd:, :] = jnp.ones((n_k, 2, vbuf.shape[2] - 2 * hd, rows), BF16)
        vbuf[n_k] = jnp.zeros(vbuf.shape[1:], BF16)
        for load in loads[:3]:
            load.wait()
        wqt[...] = wq[...].T
        wvt[...] = wv[...].T

    if not first:
        project_setup()
        for load in loads[0 if last else 3:]:
            load.wait()
        own_s.wait()
        own_p.wait()

        for buf, recv in ((rs, tr), (rp, er)):
            ref = buf.at[pl.ds(0, 7)]
            remote(ref, ref, snd.at[0], recv, partner).wait_recv()
        parts = []
        for g in range(2):
            stats = [rs[yv[i] * 2 + g] for i in range(4)]
            top = functools.reduce(jnp.maximum, [t[:4] for t in stats])
            share = [jnp.exp2(t[:4] - top) for t in stats]
            mass = functools.reduce(jnp.add, [f * t[4:] for f, t in zip(share, stats)])
            inverse = 1.0 / mass
            share = [f * inverse for f in share]
            for h in range(4):
                span = slice(h * hd, (h + 1) * hd)
                total = rp[yv[0] * 2 + g, span].astype(F32) * share[0][h:h + 1]
                for i in (1, 2, 3):
                    total = total + rp[yv[i] * 2 + g, span].astype(F32) * share[i][h:h + 1]
                parts.append(total)
        attn = jnp.concatenate(parts, axis=0).T.astype(BF16)

        def finish_layer(span):
            mixed = jnp.dot(attn[span], wout[...], preferred_element_type=F32)
            hidden = layer_norm(x_in[span].astype(F32) + mixed, gain[l - 1, 0:1], bias[l - 1, 0:1]).astype(BF16)
            up = gelu(jnp.dot(hidden, wup[...], preferred_element_type=F32)).astype(BF16)
            down = jnp.dot(up, wdown[...], preferred_element_type=F32)
            x_new = layer_norm(hidden.astype(F32) + down, gain[l - 1, 1:2], bias[l - 1, 1:2]).astype(BF16)
            if not last:
                xk[c * 16 + z * 4 + x, span] = x_new
            x_out[span] = x_new

    if last:
        finish_layer(slice(0, rows))

    if not last:
        own_slot = c * 16 + z * 4 + x
        if first:
            own.wait()

        def part(ref, h):
            return ref if h is None else ref.at[pl.ds(h * half, half)]

        def arrived(ref, recv):
            remote(ref, ref, snd.at[2], recv, partner).wait_recv()

        def sem_at(i, h):
            return 4 if i == 3 else 2 * (i - 1) + h

        def send_a(ka, h, up):
            ref = part(xk.at[c * 16 + nat(ka, 0)], h)
            to = (1 if up else 2) if ka == 0 else 3
            go(2, ref, ref, ra.at[sem_at(to, h)], dev_a(2 if up else 1))

        def wait_a(ka, h=None):
            arrived(part(xk.at[c * 16 + nat(ka, 0)], h), ra.at[sem_at(ka, h)])

        def send_b(ka, kb, h, up):
            ref = part(xk.at[c * 16 + nat(ka, kb)], h)
            to = (1 if up else 2) if kb == 0 else 3
            go(2, ref, ref, rb.at[ka, sem_at(to, h)], dev_b(2 if up else 1))

        def wait_b(ka, kb, h=None):
            arrived(part(xk.at[c * 16 + nat(ka, kb)], h), rb.at[ka, sem_at(kb, h)])

        def send_y(i, h, up):
            ref = part(xk.at[own_slot] if i == 0 else xq.at[c, yv[i]], h)
            to = (1 if up else 2) if i == 0 else 3
            go(3, ref, part(xq.at[c, yv[i]], h), ry.at[sem_at(to, h)], dev_y(2 if up else 1, c))

        def wait_y(i, h=None):
            arrived(part(xq.at[c, yv[i]], h), ry.at[sem_at(i, h)])

        def share(ka, kb):
            n = nat(ka, kb)
            go(2, xk.at[c * 16 + n], xk.at[c * 16 + n], rd.at[GROUP_OF[ka, kb]], partner)

        def share_y(i):
            ref = xq.at[c, yv[i]]
            go(3, ref, ref, rq.at[i - 1], partner)

        def project_kv(s, t):
            xs = jnp.concatenate([xk[s], xk[t]], axis=0)
            k = jnp.dot(xs, wk[...], preferred_element_type=F32).astype(BF16)
            v = lax.dot_general(wvt[...], xs, (((1,), (1,)), ((), ())), preferred_element_type=F32).astype(BF16)
            for i, to in enumerate((s, t)):
                span = slice(i * rows, (i + 1) * rows)
                kbuf[to] = k[span]
                vbuf[to, 0, :2 * hd] = v[:2 * hd, span]
                vbuf[to, 1, :2 * hd] = v[2 * hd:, span]

        def project_q(i, mine, other):
            xs = jnp.concatenate([mine, other], axis=0)
            t = lax.dot_general(wqt[...], xs, (((1,), (1,)), ((), ())), preferred_element_type=F32)
            t = (t * scale).astype(BF16)
            for j, core in enumerate((c, e)):
                span = slice(j * rows, (j + 1) * rows)
                for h in range(2):
                    base = h * 2 * hd
                    qbuf[yv[i] * 2 + core, h, :hd, :rows] = t[base:base + hd, span]
                    qbuf[yv[i] * 2 + core, h, hd:, rows:] = t[base + hd:base + 2 * hd, span]

        def finish(*blocks):
            assert blocks in GROUPS
            arrived(xk.at[pl.ds(0, len(blocks))], rd.at[GROUPS.index(blocks)])
            for ka, kb in blocks:
                project_kv(c * 16 + nat(ka, kb), e * 16 + nat_partner(ka, kb))

        def finish_y(*which):
            for i in which:
                if i == 0:
                    project_q(0, xk[own_slot], xk[e * 16 + z * 4 + x])
                else:
                    arrived(xq.at[e, yv[i]], rq.at[i - 1])
                    project_q(i, xq[c, yv[i]], xq[e, yv[i]])

        def send_own(h, up):
            send_a(0, h, up)
            send_b(0, 0, h, up)
            send_y(0, h, up)

        if not first:
            finish_layer(slice(0, rows))
        for h in (0, 1):
            send_own(h, True)
            send_own(1 - h, False)
        share(0, 0)
        if first:
            project_setup()
            own_mask.wait()
            link_pairs(masked, listed)
        finish((0, 0))
        finish_y(0)
        wait_a(1, 0)
        send_a(1, 0, True)
        send_b(1, 0, 0, True)
        wait_a(2, 1)
        send_a(2, 1, False)
        send_b(2, 0, 1, False)
        wait_b(0, 1, 0)
        send_b(0, 1, 0, True)
        wait_b(0, 2, 1)
        send_b(0, 2, 1, False)
        wait_y(1, 0)
        send_y(1, 0, True)
        wait_y(2, 1)
        send_y(2, 1, False)
        wait_a(1, 1)
        send_b(1, 0, 1, False)
        wait_a(2, 0)
        send_b(2, 0, 0, True)
        send_b(1, 0, 1, True)
        send_b(1, 0, 0, False)
        send_b(2, 0, 0, False)
        send_b(2, 0, 1, True)
        share(1, 0)
        share(2, 0)
        wait_b(0, 1, 1)
        share(0, 1)
        wait_b(0, 2, 0)
        share(0, 2)
        wait_y(1, 1)
        share_y(1)
        wait_y(2, 0)
        share_y(2)
        finish((1, 0))
        wait_a(3)
        send_b(3, 0, 0, True)
        send_b(3, 0, 1, False)
        send_b(3, 0, 1, True)
        send_b(3, 0, 0, False)
        share(3, 0)
        finish((2, 0), (0, 1))
        for ka in (1, 2):
            wait_b(ka, 1, 0)
            send_b(ka, 1, 0, True)
            wait_b(ka, 2, 1)
            send_b(ka, 2, 1, False)
        wait_b(0, 3)
        share(0, 3)
        finish((0, 2))
        finish_y(1, 2)
        for ka in (1, 2):
            wait_b(ka, 1, 1)
            share(ka, 1)
            wait_b(ka, 2, 0)
            share(ka, 2)
        wait_y(3)
        share_y(3)
        finish((3, 0))
        wait_b(3, 1, 0)
        send_b(3, 1, 0, True)
        wait_b(3, 2, 1)
        send_b(3, 2, 1, False)
        finish((0, 3), (1, 1))
        for ka in (1, 2):
            wait_b(ka, 3)
            share(ka, 3)
        wait_b(3, 1, 1)
        share(3, 1)
        wait_b(3, 2, 0)
        share(3, 2)
        finish((1, 2), (2, 1), (2, 2))
        finish_y(3)
        finish((1, 3), (2, 3))
        wait_b(3, 3)
        share(3, 3)
        finish((3, 1), (3, 2))
        finish((3, 3))

    kinds = []
    if not first:
        kinds += [(0, sin.at[pl.ds(0, 7)]), (1, pin.at[pl.ds(0, 7)])]
    if not last:
        kinds += [(2, xk.at[pl.ds(0, 31)]), (3, xk.at[pl.ds(0, 6)])]
    for kind, ref in kinds:
        remote(ref, ref, snd.at[kind], er if not first else rq.at[0], partner).wait_send()


def link_pairs(mask, out):
    x, y, z, c = coords()
    n_q, n_k = 8, 32
    lane = lax.broadcasted_iota(jnp.int32, (1, 128), 1)
    in_row, of_row = lane & 15, lane >> 4
    slot = (in_row & 1) * 16 + (of_row >> 1) * 4 + (of_row & 1) * 2 + ((in_row >> 1) & 1)
    slot = slot.astype(F32)
    base = lax.axis_index("row") * 16 + (x % 2) * 2
    linked = [jnp.where((in_row >> 2) == y, mask[pl.ds(base + (q // 2) * 4 + q % 2, 1), :], 0).astype(F32)
              for q in range(n_q)]
    upper = lax.broadcasted_iota(jnp.int32, (128, 128), 0) < lax.broadcasted_iota(jnp.int32, (128, 128), 1)
    rank = jnp.dot(jnp.concatenate(linked, axis=0).astype(BF16), jnp.where(upper, 1.0, 0.0).astype(BF16),
                   preferred_element_type=F32)
    start = jnp.zeros((1, 1), F32)
    places, pads = [], []
    for q in range(n_q):
        code = slot + float(q * n_k)
        count = jnp.sum(linked[q], axis=1, keepdims=True)
        odd = count - 2.0 * jnp.floor(count * 0.5)
        places.append(jnp.where(linked[q] > 0.0, rank[q:q + 1] + start, -1.0))
        pads.append((start + count, odd, jnp.max(jnp.where(linked[q] > 0.0, code, 0.0), axis=1, keepdims=True)))
        start = start + count + odd
    places = jnp.concatenate(places + [jnp.zeros((120, 128), F32)], axis=0).T
    for chunk in range(3):
        at = (lane + chunk * 128).astype(F32)
        code = jnp.zeros((1, 128), F32)
        filler = jnp.zeros((1, 128), F32)
        for q in range(n_q):
            hot = jnp.where(places[:, q:q + 1] == at, 1.0, 0.0).astype(BF16)
            codes = jnp.broadcast_to(slot + float(q * n_k), (8, 128)).astype(BF16)
            where, odd, last = pads[q]
            pad = jnp.where(at == where, odd, 0.0)
            code = code + jnp.dot(codes, hot, preferred_element_type=F32)[0:1] + pad * last
            filler = filler + pad
        code = code.astype(jnp.int32)
        key = code & 31
        entry = (code >> 5) * 4096 + key * 64 + jnp.where(filler > 0.0, n_k, key)
        out[chunk:chunk + 1, :] = jnp.where(at < start, entry, n_q * 4096 + n_k)
    out[3:4, :] = jnp.broadcast_to(start, (1, 128)).astype(jnp.int32)


def attend(listed, kbuf, vbuf, qbuf, pout, sout, pairs, sbuf, peak, acc, top, den, sem):
    n_q, rows = qbuf.shape[0], kbuf.shape[1]
    hd = qbuf.shape[2] // 2
    load = pltpu.make_async_copy(listed, pairs, sem)
    load.start()
    acc[...] = jnp.zeros_like(acc)
    den[...] = jnp.zeros_like(den)
    top[...] = jnp.full_like(top, FLOOR)
    load.wait()
    n = pairs[3, 0]
    units = 2 * GROUP

    def entry(i):
        return pairs[i // 128, i % 128]

    def scores(it, i):
        d, h = i // 2, i % 2
        code = [entry((it * GROUP + d) * 2 + j) for j in range(2)]
        q = jnp.minimum(code[0] // 4096, n_q - 1)
        best = []
        for j in range(2):
            k = (code[j] // 64) % 64
            s = jnp.dot(kbuf[k, :, h * 2 * hd:(h + 1) * 2 * hd], qbuf[q, h], preferred_element_type=F32)
            sbuf[i, j * rows:(j + 1) * rows] = s
            best.append(jnp.max(s, axis=0, keepdims=True))
        peak[i] = jnp.maximum(*best)

    def values(it, i):
        d, h = i // 2, i % 2
        code = [entry((it * GROUP + d) * 2 + j) for j in range(2)]
        q = code[0] // 4096
        old = top[q, h]
        new = jnp.maximum(old, peak[i])
        p = jnp.exp2(sbuf[i] - new).astype(BF16)
        v = jnp.concatenate([vbuf[code[j] % 64, h] for j in range(2)], axis=1)
        o = jnp.dot(v, p, preferred_element_type=F32)
        alpha = jnp.exp2(old - new)
        top[q, h] = new
        den[q, h] = den[q, h] * alpha + o[2 * hd:2 * hd + 1]
        for g in range(2):
            lanes = slice(g * rows, (g + 1) * rows)
            span = slice((2 * h + g) * hd, (2 * h + g + 1) * hd)
            acc[q, span] = acc[q, span] * alpha[:, lanes] + o[g * hd:(g + 1) * hd, lanes]

    for i in range(AHEAD):
        scores(0, i)

    @pl.loop(0, (n + 2 * GROUP - 1) // (2 * GROUP))
    def _(it):
        for i in range(units):
            ahead = i + AHEAD
            scores(it + ahead // units, ahead % units)
            values(it, i)

    for q in range(n_q):
        pout[q] = acc[q].astype(BF16)
        for h in range(2):
            for g in range(2):
                lanes = slice(g * rows, (g + 1) * rows)
                sout[q, 2 * h + g:2 * h + g + 1] = top[q, h, :, lanes]
                sout[q, 4 + 2 * h + g:5 + 2 * h + g] = den[q, h, :, lanes]


def solution(mesh):
    def per_device(x, mask, wqkv, wout, wup, wdown, gain, bias):
        rows, width = x.shape
        layers = wqkv.shape[0]
        cols = width // 2
        ff = wup.shape[2]
        hd = width // HEADS
        n_q, n_k = 8, 32
        vmem, any_ = pl.BlockSpec(memory_space=pltpu.VMEM), pl.BlockSpec(memory_space=pltpu.HBM)
        dma = pltpu.SemaphoreType.DMA
        shape = jax.ShapeDtypeStruct
        proj = [shape((n_k, rows, cols), BF16), shape((n_k + 1, 2, 2 * hd + 16, rows), BF16),
                shape((n_q, 2, 2 * hd, 2 * rows), BF16)]

        def call_exchange(l, x, part):
            first, last = l == 0, l == layers
            ins, specs, outs = [x], [any_ if first else vmem], []
            if first:
                ins.append(mask)
                specs.append(any_)
            else:
                ins += part
                specs += [vmem, vmem]
            if not last:
                ins.append(wqkv)
                specs.append(any_)
            if not first:
                ins += [wout, wup, wdown, gain, bias]
                specs += [any_] * 3 + [vmem] * 2
            if not last:
                outs += proj
            if first:
                outs.append(shape((8, 128), jnp.int32))
            else:
                outs.append(shape((rows, width), BF16))
            scratch = [dma((6,)), dma((4,))]
            if first:
                scratch += [pltpu.VMEM((128, 128), jnp.int32), dma]
            if not first:
                scratch += [pltpu.VMEM((width, width), BF16), pltpu.VMEM((width, ff), BF16),
                            pltpu.VMEM((ff, width), BF16),
                            pltpu.VMEM((8, cols, rows), BF16), pltpu.VMEM((8, 8, rows), F32),
                            dma, dma, dma((2,))]
            if not last:
                scratch += [pltpu.VMEM((width, cols), BF16)] * 3 + [pltpu.VMEM((cols, width), BF16)] * 2
                scratch += [pltpu.VMEM((n_k, rows, width), BF16), pltpu.VMEM((2, 4, rows, width), BF16), dma]
                scratch += [dma((5,)), dma((4, 5)), dma((len(GROUPS),)), dma((5,)), dma((3,))]
            return pl.pallas_call(
                functools.partial(exchange, l, first, last),
                out_shape=outs, in_specs=specs, out_specs=[vmem] * len(outs), scratch_shapes=scratch,
                compiler_params=pltpu.CompilerParams(
                    collective_id=l, has_side_effects=True, vmem_limit_bytes=28 * 1024 * 1024),
            )(*ins)

        def call_attend(listed, projected):
            return pl.pallas_call(
                attend,
                out_shape=[shape((n_q, cols, rows), BF16), shape((n_q, 8, rows), F32)],
                in_specs=[vmem] * 4, out_specs=[vmem, vmem],
                scratch_shapes=[
                    pltpu.SMEM((8, 128), jnp.int32),
                    pltpu.VMEM((2 * GROUP, 2 * rows, 2 * rows), F32), pltpu.VMEM((2 * GROUP, 1, 2 * rows), F32),
                    pltpu.VMEM((n_q + 1, cols, rows), F32), pltpu.VMEM((n_q + 1, 2, 1, 2 * rows), F32),
                    pltpu.VMEM((n_q + 1, 2, 1, 2 * rows), F32), dma],
                compiler_params=pltpu.CompilerParams(vmem_limit_bytes=28 * 1024 * 1024),
            )(listed, *projected)

        x = pltpu.with_memory_space_constraint(x, pltpu.HBM)
        wqkv = pltpu.with_memory_space_constraint(wqkv, pltpu.HBM)
        mask = pltpu.with_memory_space_constraint(mask, pltpu.HBM)
        *projected, listed = call_exchange(0, x, None)
        for l in range(1, layers):
            *projected, x = call_exchange(l, x, call_attend(listed, projected))
        return call_exchange(layers, x, call_attend(listed, projected))[0]

    placed = (P(("row", "col"), None), P(), P(), P(), P(), P(), P(), P())
    return jax.shard_map(
        per_device, mesh=mesh, in_specs=placed, out_specs=P(("row", "col"), None), check_vma=False
    )
```
